32 devices in a mesh: shift: 16 (over z, x, core), row: 2 (over y).
Axes of the slice: x: 2, y: 2, z: 4, core: 2. Of those that a mesh axis runs over, the one named last changes fastest.
Arguments:
- solutions: bfloat16 [32, 2, 2048, 128], P('shift', None, 'row'), may hold values from -96 to 96
Outputs:
- moments: bfloat16 [2, 8, 2048, 128], P(None, None, ('row', 'shift'))
- gram_real: float32 [1024, 1024], replicated
- gram_imag: float32 [1024, 1024], replicated
The draws below stay inside these ranges and needn't reach their ends.
All inputs are finite; a program needn't handle non-finite values.
Results may differ from the reference program's by a relative error of at most 0.0061.
Values may be sent and summed in bfloat16 or wider, within the bound.
A program may use at most 64 MiB of HBM per device.

```python
import math
import jax
import jax.numpy as jnp
from jax import lax

SOURCES = 128
PANELS = 8
SHIFTS = 32
ROWS = 2048


def spiked(entries, key, source, target, blocks, factor):
    def block_of(axis_at):
        return (jnp.arange(entries.shape[axis_at]) // (entries.shape[axis_at] // blocks)).reshape((-1,) + (1,) * (entries.ndim - 1 - axis_at))

    near = jax.random.permutation(key, blocks)[block_of(target)]
    far = (block_of(target) + blocks // 2) % blocks
    return jnp.where((block_of(source) == near) | (block_of(source) == far), factor * entries, entries)


def shard_levels(own_key, shape, cuts, smallest, high):
    def one(position, parts):
        heights = jax.random.uniform(jax.random.fold_in(jax.random.fold_in(own_key, 6), position), (parts,), jnp.float32, smallest / len(cuts), high / len(cuts))
        return jnp.repeat(jnp.exp(heights), shape[position] // parts).reshape((-1,) + (1,) * (len(shape) - position - 1))

    loudness = one(*cuts[0])
    for cut in cuts[1:]:
        loudness = loudness * one(*cut)
    return loudness


def gaussian_with(rng, dims, scale, most, pieces, heavy, held_as=jnp.bfloat16):
    drawn = scale * jax.random.normal(rng, dims, jnp.float32)
    if pieces:
        drawn = drawn * shard_levels(rng, dims, pieces, -0.22, 0.18)
    return jnp.clip(spiked(drawn, jax.random.fold_in(rng, 3), *heavy), -most, most).astype(held_as)


def setup_inputs(seed: int = 0) -> dict:
    key_of = jax.random.split(jax.random.key(seed), 2)
    solutions = gaussian_with(key_of[0], (SHIFTS, 2, ROWS, SOURCES), 16.0, 96.0, ((0, 16), (2, 2)), (0, 2, 16, 2.0))
    return {"solutions": solutions}


def coefficient_block(first_shift, shift_count, all_shifts, panels):
    indices = (first_shift + jnp.arange(shift_count, dtype=jnp.int32)).astype(jnp.float32)
    orders = jnp.arange(1, panels + 1, dtype=jnp.int32).astype(jnp.float32)
    angles = orders[:, None] * (2.0 * math.pi * (indices + 0.5) / all_shifts)[None, :]
    cos_part = jnp.cos(angles) / all_shifts
    sin_part = jnp.sin(angles) / all_shifts
    real_row = jnp.stack([cos_part, -sin_part], axis=-1)
    imag_row = jnp.stack([sin_part, cos_part], axis=-1)
    return jnp.stack([real_row, imag_row], axis=0).reshape(2 * panels, 2 * shift_count).astype(jnp.bfloat16)

def pair_product(left, right):
    width = left.shape[0] * left.shape[2]
    return jnp.einsum('krl,qrm->klqm', left.astype(jnp.float32), right.astype(jnp.float32), precision=lax.Precision.HIGHEST).reshape(width, width)

def reference(solutions):
    weights = coefficient_block(0, SHIFTS, SHIFTS, PANELS)
    flat = solutions.reshape(2 * SHIFTS, ROWS * SOURCES)
    moment_sum = jnp.dot(weights, flat, preferred_element_type=jnp.float32).reshape(2, PANELS, ROWS, SOURCES)
    moments = moment_sum.astype(jnp.bfloat16)
    real_part = moments[0]
    imag_part = moments[1]
    gram_real = pair_product(real_part, real_part) + pair_product(imag_part, imag_part)
    gram_imag = pair_product(real_part, imag_part) - pair_product(imag_part, real_part)
    factor = 1.0 / math.sqrt(ROWS)
    return (moments, gram_real * factor, gram_imag * factor)
```

```python
import functools
import math

import jax
import jax.numpy as jnp
import numpy as np
from jax import lax
from jax.experimental import pallas as pl
from jax.experimental.pallas import tpu as pltpu
from jax.sharding import PartitionSpec as P

PANELS = 8
PAIRS = PANELS * (PANELS // 2) + PANELS // 2
MESH = pl.DeviceIdType.MESH


def coefficients(all_shifts):
    indices = np.arange(all_shifts, dtype=np.float32)
    orders = np.arange(1, PANELS + 1, dtype=np.float32)
    step = (np.float32(2.0 * math.pi) * (indices + np.float32(0.5)) / np.float32(all_shifts)).astype(np.float32)
    angles = (orders[:, None] * step[None, :]).astype(np.float32).astype(np.float64)
    cos_part = np.cos(angles).astype(np.float32) / np.float32(all_shifts)
    sin_part = np.sin(angles).astype(np.float32) / np.float32(all_shifts)
    real_row = np.stack([cos_part, -sin_part], axis=-1)
    imag_row = np.stack([sin_part, cos_part], axis=-1)
    both = np.stack([real_row, imag_row], axis=0).reshape(-1)
    return both.astype(jnp.bfloat16).astype(np.float32)


def exchange(
    N, R, rows, T, factor,
    w_ref, x_ref, m_ref, ag, xs, acc, sbuf, gs, rs,
    a2a_s, a2a_r, sg_s, sg_r, rs_s, rs_r, ag_s, ag_r,
):
    X = N // 2
    Z = X // 2
    s = lax.axis_index("shift")
    r = lax.axis_index("row")
    core = lax.rem(s, 2)
    zx = s // 2
    z = zx // 2
    x = lax.rem(zx, 2)
    p = r * 2 + core
    inputs = x_ref.shape[0]
    outs = 2 * PANELS

    def remote(src, dst, ss, rr, to_s, to_r):
        return pltpu.make_async_remote_copy(
            src_ref=src, dst_ref=dst, send_sem=ss, recv_sem=rr,
            device_id={"shift": to_s, "row": to_r}, device_id_type=MESH,
        )

    partner = zx * 2 + 1 - core

    barrier = pltpu.get_barrier_semaphore()
    for i in range(1, N):
        pl.semaphore_signal(barrier, inc=1, device_id={"shift": lax.rem(s + i, N), "row": r}, device_id_type=MESH)
    for i in range(1, R):
        pl.semaphore_signal(barrier, inc=1, device_id={"shift": s, "row": lax.rem(r + i, R)}, device_id_type=MESH)
    pl.semaphore_wait(barrier, N - 1 + R - 1)

    def a2a(i):
        to = lax.rem(s + i, N)
        return remote(
            x_ref.at[:, pl.ds(pl.multiple_of(to * rows, rows), rows), :], xs.at[i],
            a2a_s.at[i], a2a_r.at[i], to, r,
        )

    def order(j):
        return 1 + lax.rem(N // 2 - 1 + j, N - 1)

    def send_one(j, c):
        a2a(order(j)).start()
        return c

    lax.fori_loop(0, N - 1, send_one, 0)

    strip = 16 if rows % 16 == 0 else rows

    def weigh(block, source, first):
        for b in range(rows // strip):
            at = slice(b * strip, (b + 1) * strip)
            parts = [block(c, at).astype(jnp.float32) for c in range(inputs)]
            for o in range(outs):
                base = o * inputs * N + source * inputs
                total = parts[0] * w_ref[base]
                for c in range(1, inputs):
                    total += parts[c] * w_ref[base + c]
                if first:
                    acc[o, at, :] = total
                else:
                    acc[o, at, :] += total

    weigh(lambda c, at: x_ref[c, pl.ds(pl.multiple_of(s * rows + at.start, strip), strip), :], s, True)

    def take_one(j, c):
        i = order(j)
        a2a(i).wait_recv()
        weigh(lambda q, at: xs[i, q, at, :], lax.rem(s - i + N, N), False)
        return c

    lax.fori_loop(0, N - 1, take_one, 0)

    def round_one(o, c):
        value = acc[o].astype(jnp.bfloat16)
        sbuf[p, o] = value
        m_ref[o] = value
        return c

    lax.fori_loop(0, outs, round_one, 0)

    done = []

    def share(slot, sem, to_s, to_r):
        return remote(sbuf.at[slot], sbuf.at[slot], sg_s.at[sem], sg_r.at[slot], to_s, to_r)

    for i in range(1, R):
        c = share(p, i, s, lax.rem(r + i, R))
        c.start()
        done.append(c)
    c = share(p, 0, partner, r)
    c.start()
    done.append(c)
    for i in range(1, R):
        slot = lax.rem(r - i + R, R) * 2 + core
        share(slot, 0, s, r).wait_recv()
        c = share(slot, R - 1 + i, partner, r)
        c.start()
        done.append(c)
    for i in range(R):
        share(lax.rem(r + i, R) * 2 + 1 - core, 0, s, r).wait_recv()

    depth = 2 * R * rows

    def pair_one(t, c):
        u = jnp.minimum(p * T + t, PAIRS - 1)
        k = lax.rem(u, PANELS)
        q = lax.rem(k + u // PANELS, PANELS)
        lr = sbuf[:, k].reshape(depth, -1)
        li = sbuf[:, PANELS + k].reshape(depth, -1)
        rr = sbuf[:, q].reshape(depth, -1)
        ri = sbuf[:, PANELS + q].reshape(depth, -1)
        dims = (((0,), (0,)), ((), ()))
        out = lax.dot_general(
            lr, jnp.concatenate([rr, ri], axis=1), dims, preferred_element_type=jnp.float32
        ) + lax.dot_general(
            li, jnp.concatenate([ri, -rr], axis=1), dims, preferred_element_type=jnp.float32
        )
        out = (out * factor).astype(jnp.bfloat16)
        cut = out.shape[0] // X
        for m in range(X):
            gs[m, t] = out[m * cut : (m + 1) * cut]
        return c

    lax.fori_loop(0, T, pair_one, 0)

    def reduce(i):
        to = lax.rem(zx + i, X)
        return remote(gs.at[to], rs.at[i], rs_s.at[i], rs_r.at[i], to * 2 + core, r)

    for j in range(X - 1):
        i = 1 + (X // 2 - 1 + j) % (X - 1)
        c = reduce(i)
        c.start()
        done.append(c)
    for i in range(1, X):
        reduce(i).wait_recv()

    def sum_one(t, c):
        total = gs[zx, t].astype(jnp.float32)
        for i in range(1, X):
            total += rs[i, t].astype(jnp.float32)
        ag[p, zx, t] = total.astype(jnp.bfloat16)
        return c

    lax.fori_loop(0, T, sum_one, 0)

    count = [0]

    def forward(pp, at, to_s, to_r):
        c = remote(ag.at[pp, at], ag.at[pp, at], ag_s.at[count[0]], ag_r.at[pp, at], to_s, to_r)
        count[0] += 1
        c.start()
        done.append(c)

    def arrive(pp, at):
        remote(ag.at[pp, at], ag.at[pp, at], ag_s.at[0], ag_r.at[pp, at], s, r).wait_recv()

    def to_rows_and_partner(at):
        for i in range(1, R):
            forward(p, at, s, lax.rem(r + i, R))
        forward(p, at, partner, r)

    other_x = (z * 2 + 1 - x) * 2 + core
    for i in range(1, Z):
        forward(p, zx, (lax.rem(z + i, Z) * 2 + x) * 2 + core, r)
    forward(p, zx, other_x, r)
    to_rows_and_partner(zx)
    for i in range(1, Z):
        at = lax.rem(z - i + Z, Z) * 2 + x
        arrive(p, at)
        forward(p, at, other_x, r)
        to_rows_and_partner(at)
    for i in range(Z):
        at = lax.rem(z - i + Z, Z) * 2 + 1 - x
        arrive(p, at)
        to_rows_and_partner(at)
    sequence = [lax.rem(z - i + Z, Z) * 2 + x for i in range(Z)]
    sequence += [lax.rem(z - i + Z, Z) * 2 + 1 - x for i in range(Z)]
    for at in sequence:
        for i in range(1, R):
            pp = lax.rem(r - i + R, R) * 2 + core
            arrive(pp, at)
            forward(pp, at, partner, r)
    for at in sequence:
        for i in range(R):
            arrive(lax.rem(r + i, R) * 2 + 1 - core, at)

    def drain(j, c):
        a2a(order(j)).wait_send()
        return c

    lax.fori_loop(0, N - 1, drain, 0)
    for c in done:
        c.wait_send()


def expand(T, ag_ref, re_ref, im_ref):
    k = pl.program_id(0)
    width = re_ref.shape[0]

    def pair(u):
        return ag_ref[u // T, :, lax.rem(u, T)].astype(jnp.float32).reshape(width, 2 * width)

    half = PANELS // 2
    for d in range(PANELS):
        q = lax.rem(k + d, PANELS)
        at = pl.ds(pl.multiple_of(q * width, width), width)
        if d < half:
            v = pair(PANELS * d + k)
            re, im = v[:, :width], v[:, width:]
        elif d == half:
            v = pair(PANELS * half + jnp.minimum(k, q))
            re, im = v[:, :width], v[:, width:]
            re, im = jnp.where(k < half, re, re.T), jnp.where(k < half, im, -im.T)
        else:
            v = pair(PANELS * (PANELS - d) + q)
            re, im = v[:, :width].T, -v[:, width:].T
        re_ref[:, at] = re
        im_ref[:, at] = im


def local(N, R, solutions):
    shifts, parts, height, width = solutions.shape
    rows = height // N
    X = N // 2
    Z = X // 2
    G = 2 * R
    T = -(-PAIRS // G)
    cut = width // X
    inputs = shifts * parts
    outs = 2 * PANELS
    factor = 1.0 / math.sqrt(height * R)
    w = jnp.asarray(coefficients(shifts * N))
    bf, dma = jnp.bfloat16, pltpu.SemaphoreType.DMA
    sends = (Z - 1) + Z + X * R + R * X
    vmem = pl.BlockSpec(memory_space=pltpu.VMEM)
    moments, parts_of_gram = pl.pallas_call(
        functools.partial(exchange, N, R, rows, T, factor),
        out_shape=(
            jax.ShapeDtypeStruct((outs, rows, width), bf),
            jax.ShapeDtypeStruct((G, X, T, cut, 2 * width), bf),
        ),
        in_specs=[pl.BlockSpec(memory_space=pltpu.SMEM), vmem],
        out_specs=(vmem, vmem),
        scratch_shapes=[
            pltpu.VMEM((N, inputs, rows, width), bf),
            pltpu.VMEM((outs, rows, width), jnp.float32),
            pltpu.VMEM((G, outs, rows, width), bf),
            pltpu.VMEM((X, T, cut, 2 * width), bf),
            pltpu.VMEM((X, T, cut, 2 * width), bf),
            dma((N,)), dma((N,)), dma((2 * R,)), dma((G,)),
            dma((X,)), dma((X,)), dma((sends,)), dma((G, X)),
        ],
        compiler_params=pltpu.CompilerParams(
            collective_id=0, has_side_effects=True, vmem_limit_bytes=40 * 2**20
        ),
        cost_estimate=pl.CostEstimate(flops=10**9, bytes_accessed=2**23, transcendentals=0),
    )(w, solutions.reshape(inputs, height, width))
    size = PANELS * width
    block = pl.BlockSpec((width, size), lambda k: (k, 0))
    gram_real, gram_imag = pl.pallas_call(
        functools.partial(expand, T),
        grid=(PANELS,),
        out_shape=(jax.ShapeDtypeStruct((size, size), jnp.float32),) * 2,
        in_specs=[vmem],
        out_specs=(block, block),
        cost_estimate=pl.CostEstimate(flops=10**7, bytes_accessed=2**24, transcendentals=0),
    )(parts_of_gram)
    return moments.reshape(2, PANELS, rows, width), gram_real, gram_imag


def solution(mesh):
    return jax.shard_map(
        functools.partial(local, mesh.shape["shift"], mesh.shape["row"]),
        mesh=mesh,
        in_specs=(P("shift", None, "row", None),),
        out_specs=(P(None, None, ("row", "shift"), None), P(), P()),
        check_vma=False,
    )
```

```python
import functools
import math

import jax
import jax.numpy as jnp
import numpy as np
from jax import lax
from jax.experimental import pallas as pl
from jax.experimental.pallas import tpu as pltpu
from jax.sharding import PartitionSpec as P

PANELS = 8
PAIRS = PANELS * (PANELS // 2) + PANELS // 2
UNITS = 2 * PAIRS
HALVES = 2
MESH = pl.DeviceIdType.MESH


def coefficients(all_shifts):
    indices = np.arange(all_shifts, dtype=np.float32)
    orders = np.arange(1, PANELS + 1, dtype=np.float32)
    step = (np.float32(2.0 * math.pi) * (indices + np.float32(0.5)) / np.float32(all_shifts)).astype(np.float32)
    angles = (orders[:, None] * step[None, :]).astype(np.float32).astype(np.float64)
    cos_part = np.cos(angles).astype(np.float32) / np.float32(all_shifts)
    sin_part = np.sin(angles).astype(np.float32) / np.float32(all_shifts)
    real_row = np.stack([cos_part, -sin_part], axis=-1)
    imag_row = np.stack([sin_part, cos_part], axis=-1)
    both = np.stack([real_row, imag_row], axis=0).reshape(-1)
    return both.astype(jnp.bfloat16).astype(np.float32)


def exchange(
    N, R, rows, T, factor,
    w_ref, x_ref, m_ref, ag, xs, acc, sbuf, gs, rs,
    a2a_s, a2a_r, sg_s, sg_r, rs_s, rs_r, ag_s, ag_r,
):
    Z = N // 4
    s = lax.axis_index("shift")
    r = lax.axis_index("row")
    core = lax.rem(s, 2)
    z = s // 4
    x = lax.rem(s // 2, 2)
    inputs = x_ref.shape[0]
    outs = 2 * PANELS
    part = rows // HALVES

    def member(x_, r_, c_):
        return (r_ * 2 + x_) * 2 + c_

    def place(z_, x_, c_):
        return (z_ * 2 + x_) * 2 + c_

    p = member(x, r, core)
    partner = place(z, x, 1 - core)
    across = place(z, 1 - x, core)

    def row_at(i):
        return lax.rem(r + i + R, R)

    def remote(src, dst, ss, rr, to_s, to_r):
        return pltpu.make_async_remote_copy(
            src_ref=src, dst_ref=dst, send_sem=ss, recv_sem=rr,
            device_id={"shift": to_s, "row": to_r}, device_id_type=MESH,
        )

    barrier = pltpu.get_barrier_semaphore()
    for i in range(1, N):
        pl.semaphore_signal(barrier, inc=1, device_id={"shift": lax.rem(s + i, N), "row": r}, device_id_type=MESH)
    for i in range(1, R):
        pl.semaphore_signal(barrier, inc=1, device_id={"shift": s, "row": row_at(i)}, device_id_type=MESH)
    pl.semaphore_wait(barrier, N - 1 + R - 1)

    def a2a(h, i):
        to = lax.rem(s + i, N)
        return remote(
            x_ref.at[:, pl.ds(pl.multiple_of(to * rows + h * part, part), part), :], xs.at[h, i],
            a2a_s.at[h, i], a2a_r.at[h, i], to, r,
        )

    def order(j):
        return 1 + lax.rem(N // 2 - 1 + j, N - 1)

    def send_one(j, c):
        a2a(j // (N - 1), order(lax.rem(j, N - 1))).start()
        return c

    lax.fori_loop(0, HALVES * (N - 1), send_one, 0)

    strip = 16 if part % 16 == 0 else part

    def weigh(block, source, first):
        for b in range(part // strip):
            at = slice(b * strip, (b + 1) * strip)
            parts = [block(c, at).astype(jnp.float32) for c in range(inputs)]
            for o in range(outs):
                base = o * inputs * N + source * inputs
                total = parts[0] * w_ref[base]
                for c in range(1, inputs):
                    total += parts[c] * w_ref[base + c]
                if first:
                    acc[o, at, :] = total
                else:
                    acc[o, at, :] += total

    def take(h, low, high):
        def take_one(j, c):
            i = order(j)
            a2a(h, i).wait_recv()
            weigh(lambda q, at: xs[h, i, q, at, :], lax.rem(s - i + N, N), False)
            return c

        lax.fori_loop(low, high, take_one, 0)

    def own(h):
        weigh(
            lambda c, at: x_ref[c, pl.ds(pl.multiple_of(s * rows + h * part + at.start, strip), strip), :],
            s, True,
        )

    def round_all(h):
        def round_one(o, c):
            value = acc[o].astype(jnp.bfloat16)
            sbuf[h, p, o] = value
            m_ref[o, h * part : (h + 1) * part, :] = value
            return c

        lax.fori_loop(0, outs, round_one, 0)

    done = []

    def spreader(view, send_sems, recv_sems):
        count = [0]

        def copy(at, slot, to_s, to_r):
            return remote(view(at, slot), view(at, slot), send_sems.at[count[0]], recv_sems.at[at, slot], to_s, to_r)

        def forward(at, slot, to_s, to_r):
            c = copy(at, slot, to_s, to_r)
            count[0] += 1
            c.start()
            done.append(c)

        def arrive(at, slot):
            remote(view(at, slot), view(at, slot), send_sems.at[0], recv_sems.at[at, slot], s, r).wait_recv()

        def spread(at):
            forward(at, p, across, r)
            for i in range(1, R):
                forward(at, p, s, row_at(i))
            forward(at, p, partner, r)

        def relay(at):
            arrive(at, member(1 - x, r, core))
            for i in range(1, R):
                arrive(at, member(x, row_at(-i), core))
            for i in range(1, R):
                first = core == 0
                slot = jnp.where(first, member(1 - x, r, core), member(x, row_at(-i), core))
                forward(at, slot, jnp.where(first, s, across), jnp.where(first, row_at(i), r))
            forward(at, member(1 - x, r, core), partner, r)
            for i in range(1, R):
                forward(at, member(x, row_at(-i), core), partner, r)

        def diagonal(at):
            for i in range(1, R):
                slot = member(1 - x, row_at(-i), core)
                arrive(at, slot)
                forward(at, slot, partner, r)

        def rest(at):
            for i in range(R):
                for o in range(2):
                    arrive(at, member(lax.rem(x + o, 2), row_at(i), 1 - core))

        return spread, relay, diagonal, rest, arrive, forward

    spread, relay, diagonal, rest, _, _ = spreader(lambda h, slot: sbuf.at[h, slot], sg_s, sg_r)
    for h in range(HALVES):
        own(h)
        if h == 0:
            take(h, 0, N - 1)
        else:
            mid = (2 * (N - 1)) // 3
            take(h, 0, mid)
            relay(h - 1)
            take(h, mid, N - 1)
        round_all(h)
        spread(h)
        if h > 0:
            diagonal(h - 1)
    relay(HALVES - 1)
    diagonal(HALVES - 1)
    for h in range(HALVES):
        rest(h)

    depth = 4 * R * rows
    first_pair = (p * T) // 2
    odd = lax.rem(p * T, 2)

    def pair_one(j, c):
        u = jnp.minimum(first_pair + j, PAIRS - 1)
        k = lax.rem(u, PANELS)
        q = lax.rem(k + u // PANELS, PANELS)
        lr = sbuf[:, :, k].reshape(depth, -1)
        li = sbuf[:, :, PANELS + k].reshape(depth, -1)
        rr = sbuf[:, :, q].reshape(depth, -1)
        ri = sbuf[:, :, PANELS + q].reshape(depth, -1)
        dims = (((0,), (0,)), ((), ()))
        out = lax.dot_general(
            lr, jnp.concatenate([rr, ri], axis=1), dims, preferred_element_type=jnp.float32
        ) + lax.dot_general(
            li, jnp.concatenate([ri, -rr], axis=1), dims, preferred_element_type=jnp.float32
        )
        out = (out * factor).astype(jnp.bfloat16)
        cut = out.shape[0] // (2 * Z)
        for half in range(2):
            for m in range(Z):
                n = half * Z + m
                gs[m, 2 * j + half + 1 - odd] = out[n * cut : (n + 1) * cut]
        return c

    lax.fori_loop(0, (T + 2) // 2 if T % 2 else T // 2, pair_one, 0)

    def reduce(i):
        to = lax.rem(z + i, Z)
        return remote(gs.at[to, pl.ds(1, T)], rs.at[i], rs_s.at[i], rs_r.at[i], place(to, x, core), r)

    for j in range(Z - 1):
        c = reduce(1 + (Z // 2 - 1 + j) % (Z - 1))
        c.start()
        done.append(c)
    for i in range(1, Z):
        reduce(i).wait_recv()

    def sum_one(t, c):
        total = gs[z, t + 1].astype(jnp.float32)
        for i in range(1, Z):
            total += rs[i, t].astype(jnp.float32)
        ag[p, z, t] = total.astype(jnp.bfloat16)
        return c

    lax.fori_loop(0, T, sum_one, 0)

    spread, relay, diagonal, rest, arrive, forward = spreader(lambda at, slot: ag.at[slot, at], ag_s, ag_r)
    for j in range(Z - 1):
        i = 1 + (Z // 2 - 1 + j) % (Z - 1)
        forward(z, p, place(lax.rem(z + i, Z), x, core), r)
    ats = [lax.rem(z + Z - i, Z) for i in range(Z)]
    for n in range(Z + 2):
        if n < Z:
            if n > 0:
                arrive(ats[n], p)
            spread(ats[n])
        if 0 <= n - 1 < Z:
            relay(ats[n - 1])
        if 0 <= n - 2 < Z:
            diagonal(ats[n - 2])
    for at in ats:
        rest(at)

    def drain(j, c):
        a2a(j // (N - 1), order(lax.rem(j, N - 1))).wait_send()
        return c

    lax.fori_loop(0, HALVES * (N - 1), drain, 0)
    for c in done:
        c.wait_send()


def expand(T, m_in, ag_ref, m_out, re_out, im_out, re_buf, im_buf, sems, m_sem):
    width = re_buf.shape[1]
    half = PANELS // 2
    keep = pltpu.make_async_copy(m_in, m_out, m_sem)
    keep.start()

    def unit(n):
        return ag_ref[n // T, :, lax.rem(n, T)].astype(jnp.float32).reshape(width // 2, 2 * width)

    def pair(u):
        return jnp.concatenate([unit(2 * u), unit(2 * u + 1)], axis=0)

    def writes(k, slot):
        at = pl.ds(pl.multiple_of(k * width, width), width)
        return (
            pltpu.make_async_copy(re_buf.at[k], re_out.at[at], sems.at[0, k]),
            pltpu.make_async_copy(im_buf.at[k], im_out.at[at], sems.at[1, k]),
        )

    def one(k, c):
        for d in range(PANELS):
            q = lax.rem(k + d, PANELS)
            at = pl.ds(pl.multiple_of(q * width, width), width)
            if d < half:
                v = pair(PANELS * d + k)
                re, im = v[:, :width], v[:, width:]
            elif d == half:
                v = pair(PANELS * half + jnp.minimum(k, q))
                re, im = v[:, :width], v[:, width:]
                re, im = jnp.where(k < half, re, re.T), jnp.where(k < half, im, -im.T)
            else:
                v = pair(PANELS * (PANELS - d) + q)
                re, im = v[:, :width].T, -v[:, width:].T
            re_buf[k, :, at] = re
            im_buf[k, :, at] = im
        for copy in writes(k, k):
            copy.start()
        return c

    lax.fori_loop(0, PANELS, one, 0)

    def finish(k, c):
        for copy in writes(k, k):
            copy.wait()
        return c

    lax.fori_loop(0, PANELS, finish, 0)
    keep.wait()


def local(N, R, solutions):
    shifts, parts, height, width = solutions.shape
    rows = height // N
    Z = N // 4
    G = 4 * R
    T = -(-UNITS // G)
    cut = width // (2 * Z)
    inputs = shifts * parts
    outs = 2 * PANELS
    part = rows // HALVES
    factor = 1.0 / math.sqrt(height * R)
    w = jnp.asarray(coefficients(shifts * N))
    bf, dma = jnp.bfloat16, pltpu.SemaphoreType.DMA
    shared = 4 * R
    vmem = pl.BlockSpec(memory_space=pltpu.VMEM)
    moments, parts_of_gram = pl.pallas_call(
        functools.partial(exchange, N, R, rows, T, factor),
        out_shape=(
            jax.ShapeDtypeStruct((outs, rows, width), bf),
            jax.ShapeDtypeStruct((G, Z, T, cut, 2 * width), bf),
        ),
        in_specs=[pl.BlockSpec(memory_space=pltpu.SMEM), vmem],
        out_specs=(vmem, vmem),
        scratch_shapes=[
            pltpu.VMEM((HALVES, N, inputs, part, width), bf),
            pltpu.VMEM((outs, part, width), jnp.float32),
            pltpu.VMEM((HALVES, G, outs, part, width), bf),
            pltpu.VMEM((Z, T + 2, cut, 2 * width), bf),
            pltpu.VMEM((Z, T, cut, 2 * width), bf),
            dma((HALVES, N)), dma((HALVES, N)), dma((HALVES * shared,)), dma((HALVES, G)),
            dma((Z,)), dma((Z,)), dma((Z * shared + Z,)), dma((Z, G)),
        ],
        compiler_params=pltpu.CompilerParams(
            collective_id=0, has_side_effects=True, vmem_limit_bytes=32 * 2**20
        ),
        cost_estimate=pl.CostEstimate(flops=10**9, bytes_accessed=2**23, transcendentals=0),
    )(w, solutions.reshape(inputs, height, width))
    size = PANELS * width
    anywhere = pl.BlockSpec(memory_space=pl.ANY)
    moments, gram_real, gram_imag = pl.pallas_call(
        functools.partial(expand, T),
        out_shape=(
            jax.ShapeDtypeStruct((outs, rows, width), bf),
            jax.ShapeDtypeStruct((size, size), jnp.float32),
            jax.ShapeDtypeStruct((size, size), jnp.float32),
        ),
        in_specs=[vmem, vmem],
        out_specs=(anywhere, anywhere, anywhere),
        scratch_shapes=[
            pltpu.VMEM((PANELS, width, size), jnp.float32),
            pltpu.VMEM((PANELS, width, size), jnp.float32),
            dma((2, PANELS)),
            dma,
        ],
        compiler_params=pltpu.CompilerParams(vmem_limit_bytes=32 * 2**20),
        cost_estimate=pl.CostEstimate(flops=10**7, bytes_accessed=2**24, transcendentals=0),
    )(moments, parts_of_gram)
    return moments.reshape(2, PANELS, rows, width), gram_real, gram_imag


def solution(mesh):
    return jax.shard_map(
        functools.partial(local, mesh.shape["shift"], mesh.shape["row"]),
        mesh=mesh,
        in_specs=(P("shift", None, "row", None),),
        out_specs=(P(None, None, ("row", "shift"), None), P(), P()),
        check_vma=False,
    )
```

```python
import functools
import math

import jax
import jax.numpy as jnp
import numpy as np
from jax import lax
from jax.experimental import pallas as pl
from jax.experimental.pallas import tpu as pltpu
from jax.sharding import PartitionSpec as P

PANELS = 8
PAIRS = PANELS * (PANELS // 2) + PANELS // 2
UNITS = 2 * PAIRS
HALVES = 2
MESH = pl.DeviceIdType.MESH


def coefficients(all_shifts):
    indices = np.arange(all_shifts, dtype=np.float32)
    orders = np.arange(1, PANELS + 1, dtype=np.float32)
    step = (np.float32(2.0 * math.pi) * (indices + np.float32(0.5)) / np.float32(all_shifts)).astype(np.float32)
    angles = (orders[:, None] * step[None, :]).astype(np.float32).astype(np.float64)
    cos_part = np.cos(angles).astype(np.float32) / np.float32(all_shifts)
    sin_part = np.sin(angles).astype(np.float32) / np.float32(all_shifts)
    real_row = np.stack([cos_part, -sin_part], axis=-1)
    imag_row = np.stack([sin_part, cos_part], axis=-1)
    both = np.stack([real_row, imag_row], axis=0).reshape(-1)
    return both.astype(jnp.bfloat16).astype(np.float32)


def exchange(
    N, R, rows, T, factor,
    w_ref, x_ref, m_ref, ag, xs, acc, sbuf, gs, rs,
    a2a_s, a2a_r, sg_s, sg_r, rs_s, rs_r, ag_s, ag_r,
):
    Z = N // 4
    s = lax.axis_index("shift")
    r = lax.axis_index("row")
    core = lax.rem(s, 2)
    z = s // 4
    x = lax.rem(s // 2, 2)
    inputs = x_ref.shape[0]
    outs = 2 * PANELS
    part = rows // HALVES

    def member(x_, r_, c_):
        return (r_ * 2 + x_) * 2 + c_

    def place(z_, x_, c_):
        return (z_ * 2 + x_) * 2 + c_

    p = member(x, r, core)
    partner = place(z, x, 1 - core)
    across = place(z, 1 - x, core)

    def row_at(i):
        return lax.rem(r + i + R, R)

    def remote(src, dst, ss, rr, to_s, to_r):
        return pltpu.make_async_remote_copy(
            src_ref=src, dst_ref=dst, send_sem=ss, recv_sem=rr,
            device_id={"shift": to_s, "row": to_r}, device_id_type=MESH,
        )

    barrier = pltpu.get_barrier_semaphore()
    for i in range(1, N):
        pl.semaphore_signal(barrier, inc=1, device_id={"shift": lax.rem(s + i, N), "row": r}, device_id_type=MESH)
    for i in range(1, R):
        pl.semaphore_signal(barrier, inc=1, device_id={"shift": s, "row": row_at(i)}, device_id_type=MESH)
    pl.semaphore_wait(barrier, N - 1 + R - 1)

    def a2a(h, i):
        to = lax.rem(s + i, N)
        return remote(
            x_ref.at[:, pl.ds(pl.multiple_of(to * rows + h * part, part), part), :], xs.at[h, i],
            a2a_s.at[h, i], a2a_r.at[h, i], to, r,
        )

    def order(j):
        return 1 + j

    def send_one(j, c):
        a2a(j // (N - 1), order(lax.rem(j, N - 1))).start()
        return c

    lax.fori_loop(0, HALVES * (N - 1), send_one, 0)

    strip = 16 if part % 16 == 0 else part

    def weigh(block, source, first):
        for b in range(part // strip):
            at = slice(b * strip, (b + 1) * strip)
            parts = [block(c, at).astype(jnp.float32) for c in range(inputs)]
            for o in range(outs):
                base = o * inputs * N + source * inputs
                total = parts[0] * w_ref[base]
                for c in range(1, inputs):
                    total += parts[c] * w_ref[base + c]
                if first:
                    acc[o, at, :] = total
                else:
                    acc[o, at, :] += total

    def take(h, low, high):
        def take_one(j, c):
            i = order(j)
            a2a(h, i).wait_recv()
            weigh(lambda q, at: xs[h, i, q, at, :], lax.rem(s - i + N, N), False)
            return c

        lax.fori_loop(low, high, take_one, 0)

    def own(h):
        weigh(
            lambda c, at: x_ref[c, pl.ds(pl.multiple_of(s * rows + h * part + at.start, strip), strip), :],
            s, True,
        )

    def round_all(h):
        def round_one(o, c):
            value = acc[o].astype(jnp.bfloat16)
            sbuf[h, p, o] = value
            m_ref[o, h * part : (h + 1) * part, :] = value
            return c

        lax.fori_loop(0, outs, round_one, 0)

    done = []

    def spreader(view, send_sems, recv_sems):
        count = [0]

        def copy(at, slot, to_s, to_r):
            return remote(view(at, slot), view(at, slot), send_sems.at[count[0]], recv_sems.at[at, slot], to_s, to_r)

        def forward(at, slot, to_s, to_r):
            c = copy(at, slot, to_s, to_r)
            count[0] += 1
            c.start()
            done.append(c)

        def arrive(at, slot):
            remote(view(at, slot), view(at, slot), send_sems.at[0], recv_sems.at[at, slot], s, r).wait_recv()

        def spread(at):
            forward(at, p, across, r)
            for i in range(1, R):
                forward(at, p, s, row_at(i))
            forward(at, p, partner, r)

        def relay(at):
            arrive(at, member(1 - x, r, core))
            for i in range(1, R):
                arrive(at, member(x, row_at(-i), core))
            for i in range(1, R):
                first = core == 0
                slot = jnp.where(first, member(1 - x, r, core), member(x, row_at(-i), core))
                forward(at, slot, jnp.where(first, s, across), jnp.where(first, row_at(i), r))
            forward(at, member(1 - x, r, core), partner, r)
            for i in range(1, R):
                forward(at, member(x, row_at(-i), core), partner, r)

        def diagonal(at):
            for i in range(1, R):
                slot = member(1 - x, row_at(-i), core)
                arrive(at, slot)
                forward(at, slot, partner, r)

        def rest(at):
            for i in range(R):
                for o in range(2):
                    arrive(at, member(lax.rem(x + o, 2), row_at(i), 1 - core))

        return spread, relay, diagonal, rest, arrive, forward

    spread, relay, diagonal, rest, _, _ = spreader(lambda h, slot: sbuf.at[h, slot], sg_s, sg_r)
    for h in range(HALVES):
        own(h)
        if h == 0:
            take(h, 0, N - 1)
        else:
            mid = (2 * (N - 1)) // 3
            take(h, 0, mid)
            relay(h - 1)
            take(h, mid, N - 1)
        round_all(h)
        spread(h)
        if h > 0:
            diagonal(h - 1)
    relay(HALVES - 1)
    diagonal(HALVES - 1)
    for h in range(HALVES):
        rest(h)

    depth = 4 * R * rows
    first_pair = (p * T) // 2
    odd = lax.rem(p * T, 2)

    def pair_one(j, c):
        u = jnp.minimum(first_pair + j, PAIRS - 1)
        k = lax.rem(u, PANELS)
        q = lax.rem(k + u // PANELS, PANELS)
        lr = sbuf[:, :, k].reshape(depth, -1)
        li = sbuf[:, :, PANELS + k].reshape(depth, -1)
        rr = sbuf[:, :, q].reshape(depth, -1)
        ri = sbuf[:, :, PANELS + q].reshape(depth, -1)
        dims = (((0,), (0,)), ((), ()))
        out = lax.dot_general(
            lr, jnp.concatenate([rr, ri], axis=1), dims, preferred_element_type=jnp.float32
        ) + lax.dot_general(
            li, jnp.concatenate([ri, -rr], axis=1), dims, preferred_element_type=jnp.float32
        )
        out = (out * factor).astype(jnp.bfloat16)
        cut = out.shape[0] // (2 * Z)
        for half in range(2):
            for m in range(Z):
                n = half * Z + m
                gs[m, 2 * j + half + 1 - odd] = out[n * cut : (n + 1) * cut]
        return c

    lax.fori_loop(0, (T + 2) // 2 if T % 2 else T // 2, pair_one, 0)

    def reduce(i):
        to = lax.rem(z + i, Z)
        return remote(gs.at[to, pl.ds(1, T)], rs.at[i], rs_s.at[i], rs_r.at[i], place(to, x, core), r)

    for j in range(Z - 1):
        c = reduce(1 + (Z // 2 - 1 + j) % (Z - 1))
        c.start()
        done.append(c)
    for i in range(1, Z):
        reduce(i).wait_recv()

    def sum_one(t, c):
        total = gs[z, t + 1].astype(jnp.float32)
        for i in range(1, Z):
            total += rs[i, t].astype(jnp.float32)
        ag[p, z, t] = total.astype(jnp.bfloat16)
        return c

    lax.fori_loop(0, T, sum_one, 0)

    spread, relay, diagonal, rest, arrive, forward = spreader(lambda at, slot: ag.at[slot, at], ag_s, ag_r)
    def mate(m):
        if Z & (Z - 1):
            return lax.rem(z + m, Z), lax.rem(z + Z - m, Z)
        out = z
        for b in range(m.bit_length()):
            if m >> b & 1:
                out = out + (1 - 2 * lax.rem(z // (1 << b), 2)) * (1 << b)
        return out, out

    for m in range(1, Z):
        forward(z, p, place(mate(m)[0], x, core), r)
    ats = [z] + [mate(m)[1] for m in range(1, Z)]
    for n in range(Z + 2):
        if n < Z:
            if n > 0:
                arrive(ats[n], p)
            spread(ats[n])
        if 0 <= n - 1 < Z:
            relay(ats[n - 1])
        if 0 <= n - 2 < Z:
            diagonal(ats[n - 2])
    for at in ats:
        rest(at)

    def drain(j, c):
        a2a(j // (N - 1), order(lax.rem(j, N - 1))).wait_send()
        return c

    lax.fori_loop(0, HALVES * (N - 1), drain, 0)
    for c in done:
        c.wait_send()


def expand(T, m_in, ag_ref, m_out, re_out, im_out, re_buf, im_buf, sems, m_sem):
    width = re_buf.shape[1]
    half = PANELS // 2
    keep = pltpu.make_async_copy(m_in, m_out, m_sem)
    keep.start()

    def unit(n):
        return ag_ref[n // T, :, lax.rem(n, T)].astype(jnp.float32).reshape(width // 2, 2 * width)

    def pair(u):
        return jnp.concatenate([unit(2 * u), unit(2 * u + 1)], axis=0)

    def writes(k, slot):
        at = pl.ds(pl.multiple_of(k * width, width), width)
        return (
            pltpu.make_async_copy(re_buf.at[k], re_out.at[at], sems.at[0, k]),
            pltpu.make_async_copy(im_buf.at[k], im_out.at[at], sems.at[1, k]),
        )

    def one(k, c):
        for d in range(PANELS):
            q = lax.rem(k + d, PANELS)
            at = pl.ds(pl.multiple_of(q * width, width), width)
            if d < half:
                v = pair(PANELS * d + k)
                re, im = v[:, :width], v[:, width:]
            elif d == half:
                v = pair(PANELS * half + jnp.minimum(k, q))
                re, im = v[:, :width], v[:, width:]
                re, im = jnp.where(k < half, re, re.T), jnp.where(k < half, im, -im.T)
            else:
                v = pair(PANELS * (PANELS - d) + q)
                re, im = v[:, :width].T, -v[:, width:].T
            re_buf[k, :, at] = re
            im_buf[k, :, at] = im
        for copy in writes(k, k):
            copy.start()
        return c

    lax.fori_loop(0, PANELS, one, 0)

    def finish(k, c):
        for copy in writes(k, k):
            copy.wait()
        return c

    lax.fori_loop(0, PANELS, finish, 0)
    keep.wait()


def local(N, R, solutions):
    shifts, parts, height, width = solutions.shape
    rows = height // N
    Z = N // 4
    G = 4 * R
    T = -(-UNITS // G)
    cut = width // (2 * Z)
    inputs = shifts * parts
    outs = 2 * PANELS
    part = rows // HALVES
    factor = 1.0 / math.sqrt(height * R)
    w = jnp.asarray(coefficients(shifts * N))
    bf, dma = jnp.bfloat16, pltpu.SemaphoreType.DMA
    shared = 4 * R
    vmem = pl.BlockSpec(memory_space=pltpu.VMEM)
    moments, parts_of_gram = pl.pallas_call(
        functools.partial(exchange, N, R, rows, T, factor),
        out_shape=(
            jax.ShapeDtypeStruct((outs, rows, width), bf),
            jax.ShapeDtypeStruct((G, Z, T, cut, 2 * width), bf),
        ),
        in_specs=[pl.BlockSpec(memory_space=pltpu.SMEM), vmem],
        out_specs=(vmem, vmem),
        scratch_shapes=[
            pltpu.VMEM((HALVES, N, inputs, part, width), bf),
            pltpu.VMEM((outs, part, width), jnp.float32),
            pltpu.VMEM((HALVES, G, outs, part, width), bf),
            pltpu.VMEM((Z, T + 2, cut, 2 * width), bf),
            pltpu.VMEM((Z, T, cut, 2 * width), bf),
            dma((HALVES, N)), dma((HALVES, N)), dma((HALVES * shared,)), dma((HALVES, G)),
            dma((Z,)), dma((Z,)), dma((Z * shared + Z,)), dma((Z, G)),
        ],
        compiler_params=pltpu.CompilerParams(
            collective_id=0, has_side_effects=True, vmem_limit_bytes=32 * 2**20
        ),
        cost_estimate=pl.CostEstimate(flops=10**9, bytes_accessed=2**23, transcendentals=0),
    )(w, solutions.reshape(inputs, height, width))
    size = PANELS * width
    anywhere = pl.BlockSpec(memory_space=pl.ANY)
    moments, gram_real, gram_imag = pl.pallas_call(
        functools.partial(expand, T),
        out_shape=(
            jax.ShapeDtypeStruct((outs, rows, width), bf),
            jax.ShapeDtypeStruct((size, size), jnp.float32),
            jax.ShapeDtypeStruct((size, size), jnp.float32),
        ),
        in_specs=[vmem, vmem],
        out_specs=(anywhere, anywhere, anywhere),
        scratch_shapes=[
            pltpu.VMEM((PANELS, width, size), jnp.float32),
            pltpu.VMEM((PANELS, width, size), jnp.float32),
            dma((2, PANELS)),
            dma,
        ],
        compiler_params=pltpu.CompilerParams(vmem_limit_bytes=32 * 2**20),
        cost_estimate=pl.CostEstimate(flops=10**7, bytes_accessed=2**24, transcendentals=0),
    )(moments, parts_of_gram)
    return moments.reshape(2, PANELS, rows, width), gram_real, gram_imag


def solution(mesh):
    return jax.shard_map(
        functools.partial(local, mesh.shape["shift"], mesh.shape["row"]),
        mesh=mesh,
        in_specs=(P("shift", None, "row", None),),
        out_specs=(P(None, None, ("row", "shift"), None), P(), P()),
        check_vma=False,
    )
```
